64 devices in a mesh: dp: 4 (over x, y), sp: 16 (over z, core).
Axes of the slice: x: 2, y: 2, z: 8, core: 2. Of those that a mesh axis runs over, the one named last changes fastest.
The devices are a block of a 4x4x8 slice.
Arguments:
- x: bfloat16 [24576, 2048], P(('dp', 'sp')), parts along dimension 0
- wq: bfloat16 [2048, 2048], replicated
- wk: bfloat16 [2048, 2048], replicated
- wv: bfloat16 [2048, 2048], replicated
- wo: bfloat16 [2048, 2048], replicated
- idx: int32 [24576, 6], P(('dp', 'sp')), parts along dimension 0
- probs: float32 [24576, 64], P(('dp', 'sp')), parts along dimension 0
Outputs:
- output 1: bfloat16 [24576, 2048], P(('dp', 'sp')), parts along dimension 0
- output 2: bfloat16 [256, 1152, 2048], P(('dp', 'sp')), parts along dimension 0
There are 4 independent parts. The reference program is written for one: setup_inputs(seed, part) draws one part's arguments, and reference() takes and returns one part's arrays. A program takes and returns all parts, laid end to end along the dimension named above; an argument that names none is the same for every part.
All inputs are finite; a program needn't handle non-finite values.
Results may differ from the reference program's by a relative error of at most 0.00321.
Values are sent between devices in bfloat16 or wider.
A program may use at most 768 MiB of HBM per device.

```python
import math
import jax
import jax.numpy as jnp
from jax import lax

H = 2048
HEADS = 16
KV_HEADS = 16
HEAD = 128
EXPERTS = 64
TOP = 6
SEQ = 6144
GROUP = 16
CAP = 72
ROPE_BASE = 1000000.0
QBLK = min(SEQ, 128)


def setup_inputs(seed: int = 0, part: int = 0) -> dict:
    key = jax.random.key(seed)
    kw = jax.random.split(key, 4)
    kd = jax.random.split(jax.random.fold_in(key, part), 3)
    ke = jax.random.split(jax.random.fold_in(jax.random.fold_in(key, part), 7), 2)
    sq = math.sqrt(math.log(max(SEQ / 16.0, 2.0)))
    x = jax.random.normal(kd[0], (SEQ, H), jnp.float32)
    wq = jax.random.normal(kw[0], (H, HEADS * HEAD), jnp.float32) * (sq / math.sqrt(H))
    wk = jax.random.normal(kw[1], (H, KV_HEADS * HEAD), jnp.float32) * (1.0 / math.sqrt(H))
    wv = jax.random.normal(kw[2], (H, KV_HEADS * HEAD), jnp.float32) * (1.0 / math.sqrt(H))
    wo = jax.random.normal(kw[3], (HEADS * HEAD, H), jnp.float32) * (1.0 / math.sqrt(HEADS * HEAD))
    normal_sum = jnp.sum(jax.random.randint(ke[0], (12, EXPERTS), 0, 256, jnp.int32), axis=0) * 2 - 12 * 255
    quarter_log = jnp.clip((normal_sum * 35) >> 11, -28, 28) + 28
    shift_part = (quarter_log >> 2).astype(jnp.uint32)
    mantissa = (8 - (quarter_log & 3)).astype(jnp.uint32)
    wait_time = ((jax.random.bits(ke[1], (SEQ, EXPERTS), jnp.uint32) >> 5) * mantissa[None, :]) >> shift_part[None, :]
    idx = jnp.argsort(wait_time, axis=1)[:, :TOP].astype(jnp.int32)
    probs = jax.nn.softmax(jax.random.normal(kd[2], (SEQ, EXPERTS), jnp.float32), axis=1)
    return {"x": x.astype(jnp.bfloat16), "wq": wq.astype(jnp.bfloat16), "wk": wk.astype(jnp.bfloat16), "wv": wv.astype(jnp.bfloat16), "wo": wo.astype(jnp.bfloat16), "idx": idx, "probs": probs}


def rope(t, pos):
    half = HEAD // 2
    inv = ROPE_BASE ** (-jnp.arange(half, dtype=jnp.float32) * (2.0 / HEAD))
    ang = pos.astype(jnp.float32)[:, None] * inv[None, :]
    c = jnp.cos(ang)[:, None, :]
    s = jnp.sin(ang)[:, None, :]
    a = t[..., :half]
    b = t[..., half:]
    return jnp.concatenate([a * c - b * s, b * c + a * s], axis=-1)


def reference(x, wq, wk, wv, wo, idx, probs):
    m = HEADS // KV_HEADS
    pos = jnp.arange(SEQ)
    q = rope(jnp.dot(x, wq, preferred_element_type=jnp.float32).reshape(SEQ, HEADS, HEAD), pos).astype(jnp.bfloat16)
    k = rope(jnp.dot(x, wk, preferred_element_type=jnp.float32).reshape(SEQ, KV_HEADS, HEAD), pos).astype(jnp.bfloat16)
    v = jnp.dot(x, wv, preferred_element_type=jnp.float32).astype(jnp.bfloat16).reshape(SEQ, KV_HEADS, HEAD)
    qg = q.reshape(SEQ, KV_HEADS, m, HEAD).transpose(1, 2, 0, 3)
    kg = k.transpose(1, 0, 2)
    vg = v.transpose(1, 0, 2)
    nb = SEQ // QBLK
    scale = 1.0 / math.sqrt(HEAD)

    def group(a):
        qh, kh, vh = a
        qs = qh.reshape(m, nb, QBLK, HEAD).transpose(1, 0, 2, 3)
        kf = kh.astype(jnp.float32)
        vf = vh.astype(jnp.float32)

        def block(b):
            qq, j = b
            sc = jnp.einsum("iqd,kd->iqk", qq.astype(jnp.float32), kf) * scale
            qpos = j * QBLK + jnp.arange(QBLK)
            keep = pos[None, :] <= qpos[:, None]
            sc = jnp.where(keep[None], sc, -jnp.inf)
            p = jax.nn.softmax(sc, axis=-1).astype(jnp.bfloat16)
            return jnp.einsum("iqk,kd->iqd", p.astype(jnp.float32), vf).astype(jnp.bfloat16)

        ob = lax.map(block, (qs, jnp.arange(nb)))
        return ob.transpose(1, 0, 2, 3).reshape(m, SEQ, HEAD)

    o = lax.map(group, (qg, kg, vg))
    o = o.transpose(2, 0, 1, 3).reshape(SEQ, HEADS * HEAD)
    h = (x.astype(jnp.float32) + jnp.dot(o, wo, preferred_element_type=jnp.float32)).astype(jnp.bfloat16)

    sd = SEQ // GROUP
    sel = jnp.take_along_axis(probs, idx, axis=1)
    w = sel / jnp.sum(sel, axis=1, keepdims=True)
    e = idx.reshape(GROUP, sd * TOP)
    hot = (e[:, :, None] == jnp.arange(EXPERTS)[None, None, :]).astype(jnp.int32)
    rank = jnp.sum(jnp.cumsum(hot, axis=1) * hot, axis=2) - 1
    dest = e * (GROUP * CAP) + jnp.arange(GROUP)[:, None] * CAP + rank
    dest = jnp.where(rank < CAP, dest, EXPERTS * GROUP * CAP).reshape(SEQ * TOP)
    rows = (w[:, :, None] * h[:, None, :].astype(jnp.float32)).astype(jnp.bfloat16).reshape(SEQ * TOP, H)
    buf = jnp.zeros((EXPERTS * GROUP * CAP, H), jnp.bfloat16).at[dest].set(rows, mode="drop")
    return h, buf.reshape(EXPERTS, GROUP * CAP, H)
```

```python
import functools
import math
import jax
import jax.numpy as jnp
from jax import lax
from jax.experimental import pallas as pl
from jax.experimental.pallas import tpu as pltpu
from jax.sharding import PartitionSpec as P

HEAD = 128
ROPE_BASE = 1000000.0
MESH = pl.DeviceIdType.MESH
ANY = pl.BlockSpec(memory_space=pl.ANY)
VM = pl.BlockSpec(memory_space=pltpu.VMEM)
DMA = pltpu.SemaphoreType.DMA
VMEM_BYTES = 64 * 1024 * 1024 - 64 * 1024


class Ring:
    def __init__(self, n):
        self.chips = n // 2
        self.half = self.chips // 2
        self.me = lax.axis_index("sp")
        self.z = self.me // 2
        self.c = self.me % 2
        self.right = self.at(1)
        self.left = self.at(-1)
        self.part = self.z * 2 + 1 - self.c

    def at(self, d, other=False):
        c = 1 - self.c if other else self.c
        return lax.rem(self.z + self.chips + d, self.chips) * 2 + c

    def barrier(self):
        bar = pltpu.get_barrier_semaphore()
        for dev in (self.right, self.left, self.part):
            pl.semaphore_signal(bar, inc=1, device_id={"sp": dev}, device_id_type=MESH)
        pl.semaphore_wait(bar, 3)


def remote(src, dst, ss, rs, dev):
    return pltpu.make_async_remote_copy(src_ref=src, dst_ref=dst, send_sem=ss, recv_sem=rs, device_id={"sp": dev}, device_id_type=MESH)


def gather_project(n, pieces, x, wq, wk, wv, inv, meta, xf, qo, ko, vo, mo, xs, wb, qs, ks, vs, ms, cws, cwr, ccs, ccr, pts, ptr, wsem, osem):
    r = Ring(n)
    me, half = r.me, r.half
    sd, hid = x.shape
    rows = sd // pieces
    cols = pl.ds(pl.multiple_of(me * HEAD, HEAD), HEAD)
    own = [pltpu.make_async_copy(w.at[:, cols], wb.at[:, pl.ds(i * HEAD, HEAD)], wsem.at[i]) for i, w in enumerate((wq, wk, wv))]
    own.append(pltpu.make_async_copy(x, xs.at[me], wsem.at[3]))
    own.append(pltpu.make_async_copy(meta, ms.at[me], wsem.at[4]))
    for cp in own:
        cp.start()
    r.barrier()

    def blk(chunk, p):
        return ms.at[chunk] if p == pieces else xs.at[chunk, pl.ds(p * rows, rows)]

    def src(p):
        return meta if p == pieces else x.at[pl.ds(p * rows, rows)]

    sent = []

    def go(cp):
        cp.start()
        sent.append(cp)

    order = [pieces] + list(range(pieces))

    def takes(d, p, cw):
        if d < half:
            return True
        return d == half and (cw if p == pieces else (p < pieces // 2) == cw)

    for p in order:
        go(remote(src(p), blk(me, p), cws.at[0, p], cwr.at[0, p], r.right))
        go(remote(src(p), blk(me, p), ccs.at[0, p], ccr.at[0, p], r.left))
        go(remote(src(p), blk(me, p), pts.at[0, p], ptr.at[0, p], r.part))

    outs = []

    def out(src_, dst, i, slot):
        cp = pltpu.make_async_copy(src_, dst, osem.at[i, slot])
        cp.start()
        outs.append(cp)

    def project(chunk, slot):
        out(xs.at[chunk], xf.at[chunk], 0, slot)
        acc = jnp.dot(xs[chunk], wb[...], preferred_element_type=jnp.float32)
        pos = (chunk * sd + lax.broadcasted_iota(jnp.int32, (sd, HEAD), 0)).astype(jnp.float32)
        ang = pos * inv[...]
        co = jnp.cos(ang)
        si = jnp.sin(ang)
        si = jnp.where(lax.broadcasted_iota(jnp.int32, (sd, HEAD), 1) < HEAD // 2, -si, si)
        q = acc[:, :HEAD]
        k = acc[:, HEAD : 2 * HEAD]
        qs[chunk] = (q * co + pltpu.roll(q, HEAD // 2, 1) * si).astype(jnp.bfloat16)
        ks[chunk] = (k * co + pltpu.roll(k, HEAD // 2, 1) * si).astype(jnp.bfloat16)
        vs[chunk] = acc[:, 2 * HEAD :].astype(jnp.bfloat16)
        out(qs.at[chunk], qo.at[chunk], 1, slot)
        out(ks.at[chunk], ko.at[chunk], 2, slot)
        out(vs.at[chunk], vo.at[chunk], 3, slot)

    for cp in own:
        cp.wait()
    project(me, 0)
    slot = 1
    waiting = [(r.part, 0, order)]
    for d in range(1, half + 1):
        a, b = r.at(-d), r.at(d)
        s1 = 2 * d - 1
        s2 = 2 * d if d < half else s1
        for p in order:
            if takes(d, p, True):
                remote(blk(a, p), blk(a, p), cws.at[d - 1, p], cwr.at[d - 1, p], r.right).wait_recv()
                if takes(d + 1, p, True):
                    go(remote(blk(a, p), blk(a, p), cws.at[d, p], cwr.at[d, p], r.right))
                go(remote(blk(a, p), blk(a, p), pts.at[s1, p], ptr.at[s1, p], r.part))
            if takes(d, p, False):
                remote(blk(b, p), blk(b, p), ccs.at[d - 1, p], ccr.at[d - 1, p], r.left).wait_recv()
                if takes(d + 1, p, False):
                    go(remote(blk(b, p), blk(b, p), ccs.at[d, p], ccr.at[d, p], r.left))
                go(remote(blk(b, p), blk(b, p), pts.at[s2, p], ptr.at[s2, p], r.part))
        for chunk in (a, b) if d < half else (a,):
            project(chunk, slot)
            slot += 1
        for chunk, s, ps in waiting:
            for p in ps:
                remote(blk(chunk, p), blk(chunk, p), pts.at[s, p], ptr.at[s, p], r.part).wait_recv()
            project(chunk, slot)
            slot += 1
        ao, bo = r.at(-d, True), r.at(d, True)
        waiting = [(ao, s1, order), (bo, s2, order)] if d < half else [(ao, s1, order)]
    for chunk, s, ps in waiting:
        for p in ps:
            remote(blk(chunk, p), blk(chunk, p), pts.at[s, p], ptr.at[s, p], r.part).wait_recv()
        project(chunk, slot)
        slot += 1
    last = pltpu.make_async_copy(ms, mo, wsem.at[5])
    last.start()
    for cp in sent:
        cp.wait_send()
    for cp in outs:
        cp.wait()
    last.wait()


def call_gather_project(x, wq, wk, wv, inv, meta, n, pieces=4):
    sd, hid = x.shape
    half = n // 4
    bf = jnp.bfloat16
    head = jax.ShapeDtypeStruct((n, sd, HEAD), bf)
    return pl.pallas_call(
        functools.partial(gather_project, n, pieces),
        out_shape=(jax.ShapeDtypeStruct((n, sd, hid), bf), head, head, head, jax.ShapeDtypeStruct((n,) + meta.shape, meta.dtype)),
        in_specs=[ANY, ANY, ANY, ANY, VM, ANY],
        out_specs=(ANY,) * 5,
        scratch_shapes=[
            pltpu.VMEM((n, sd, hid), bf),
            pltpu.VMEM((hid, 3 * HEAD), bf),
            pltpu.VMEM((n, sd, HEAD), bf),
            pltpu.VMEM((n, sd, HEAD), bf),
            pltpu.VMEM((n, sd, HEAD), bf),
            pltpu.VMEM((n,) + meta.shape, meta.dtype),
        ]
        + [DMA((half, pieces + 1))] * 4
        + [DMA((2 * half, pieces + 1))] * 2
        + [DMA((6,)), DMA((4, n))],
        compiler_params=pltpu.CompilerParams(collective_id=1, has_side_effects=True, vmem_limit_bytes=VMEM_BYTES),
        name="gather_project",
    )(x, wq, wk, wv, inv, meta)


def attend_block(i, q, kb, vb, m, l, acc, scale):
    bq = q.shape[0]
    bk = 2 * bq
    sub = 128
    c = scale * math.log2(math.e)
    m[...] = jnp.full(m.shape, -jnp.inf, jnp.float32)
    l[...] = jnp.zeros(l.shape, jnp.float32)
    acc[...] = jnp.zeros(acc.shape, jnp.float32)

    def step(j, masked):
        ks = kb[pl.ds(pl.multiple_of(j * bk, bk), bk), :]
        vs = vb[pl.ds(pl.multiple_of(j * bk, bk), bk), :]
        for t in range(bq // sub):
            rows = pl.ds(t * sub, sub)
            s = lax.dot_general(q[rows, :], ks, (((1,), (1,)), ((), ())), preferred_element_type=jnp.float32)
            if masked:
                qp = i * bq + t * sub + lax.broadcasted_iota(jnp.int32, (sub, bk), 0)
                kp = j * bk + lax.broadcasted_iota(jnp.int32, (sub, bk), 1)
                s = jnp.where(kp <= qp, s, -jnp.inf)
            top = jnp.max(s, axis=1, keepdims=True)
            old = m[rows, :]
            new = jnp.maximum(old, top)
            p = jnp.exp2(s * c - new[:, :1] * c)
            alpha = jnp.exp2((old - new) * c)
            part = p[:, :HEAD]
            for g in range(1, bk // HEAD):
                part = part + p[:, g * HEAD : (g + 1) * HEAD]
            l[rows, :] = l[rows, :] * alpha + part
            acc[rows, :] = acc[rows, :] * alpha + jnp.dot(p.astype(jnp.bfloat16), vs, preferred_element_type=jnp.float32)
            m[rows, :] = new

    def body(j, carry):
        step(j, False)
        return carry

    lax.fori_loop(0, i // 2, body, 0)
    step(i // 2, True)
    return (acc[...] / jnp.sum(l[...], axis=1, keepdims=True)).astype(jnp.bfloat16)


def attend_gather(n, q, k, v, xf, wo, hf, o, wb, qb, kb, vb, xb, hb, m, l, acc, cws, cwr, ccs, ccr, pts, ptr, lsem, xsem, hsem):
    r = Ring(n)
    me, half = r.me, r.half
    nb, _, bq, _ = o.shape
    hid = wo.shape[1]
    cut = bq // 2
    tile = 512
    scale = 1.0 / math.sqrt(HEAD)
    load = [pltpu.make_async_copy(a, b, lsem.at[i]) for i, (a, b) in enumerate(((q, qb), (k, kb), (v, vb), (wo, wb)))]
    for cp in load:
        cp.start()
    pltpu.make_async_copy(xf.at[0], xb.at[0], xsem.at[0]).start()
    r.barrier()
    for cp in load[:3]:
        cp.wait()

    lo, hi, whole = pl.ds(0, cut), pl.ds(cut, cut), pl.ds(0, bq)

    def cw(b, d):
        chunk = r.at(-d)
        ref = o.at[b, chunk, lo if d + 1 == half else whole]
        return remote(ref, ref, cws.at[d, b], cwr.at[d, b], r.right)

    def ccw(b, d):
        chunk = r.at(d)
        ref = o.at[b, chunk, hi if d + 1 == half else whole]
        return remote(ref, ref, ccs.at[d, b], ccr.at[d, b], r.left)

    def cw_in(b, d):
        ref = o.at[b, r.at(-d), lo if d == half else whole]
        return remote(ref, ref, cws.at[d - 1, b], cwr.at[d - 1, b], r.right)

    def ccw_in(b, d):
        ref = o.at[b, r.at(d), hi if d == half else whole]
        return remote(ref, ref, ccs.at[d - 1, b], ccr.at[d - 1, b], r.left)

    def cross(b, s, other):
        d = (s + 1) // 2
        sign = -1 if s % 2 == 1 else 1
        rows = whole if d < half else (lo if sign < 0 else hi)
        ref = o.at[b, r.at(sign * d, other), rows]
        return remote(ref, ref, pts.at[s, b], ptr.at[s, b], r.part)

    def attend(i):
        o[i, me] = attend_block(i, qb.at[pl.ds(pl.multiple_of(i * bq, bq), bq)], kb, vb, m, l, acc, scale)

    def project(b):
        @pl.when(b + 1 < nb)
        def _():
            pltpu.make_async_copy(xf.at[b + 1], xb.at[(b + 1) % 2], xsem.at[(b + 1) % 2]).start()

        pltpu.make_async_copy(xf.at[b], xb.at[b % 2], xsem.at[b % 2]).wait()

        @pl.when(b >= 2)
        def _():
            pltpu.make_async_copy(hb.at[b % 2], hf.at[b - 2], hsem.at[b % 2]).wait()

        def cols(t, carry):
            at = pl.ds(pl.multiple_of(t * tile, tile), tile)
            lhs = jnp.concatenate([o[b, j] for j in range(n)], axis=1)
            y = jnp.dot(lhs, wb[:, at], preferred_element_type=jnp.float32)
            hb[b % 2, :, at] = (xb[b % 2, :, at].astype(jnp.float32) + y).astype(jnp.bfloat16)
            return carry

        lax.fori_loop(0, hid // tile, cols, 0)
        pltpu.make_async_copy(hb.at[b % 2], hf.at[b], hsem.at[b % 2]).start()

    attend(0)
    load[3].wait()

    def step(i, carry):
        @pl.when(i < nb)
        def _():
            cw(i, 0).start()
            ccw(i, 0).start()
            cross(i, 0, False).start()

        for d in range(half, 0, -1):
            b = i - d

            @pl.when(jnp.logical_and(b >= 0, b < nb))
            def _(d=d, b=b):
                cw_in(b, d).wait_recv()
                if d < half:
                    cw(b, d).start()
                cross(b, 2 * d - 1, False).start()
                ccw_in(b, d).wait_recv()
                if d < half:
                    ccw(b, d).start()
                cross(b, 2 * d, False).start()

        @pl.when(i + 1 < nb)
        def _():
            attend(i + 1)

        b = i - half - 1

        @pl.when(b >= 0)
        def _():
            for s in range(2 * half + 1):
                cross(b, s, True).wait_recv()
            project(b)

        return carry

    lax.fori_loop(0, nb + half + 1, step, 0)

    def drain(b, carry):
        for d in range(half):
            cw(b, d).wait_send()
            ccw(b, d).wait_send()
        for s in range(2 * half + 1):
            cross(b, s, False).wait_send()
        return carry

    lax.fori_loop(0, nb, drain, 0)
    for b in (nb - 2, nb - 1):
        pltpu.make_async_copy(hb.at[b % 2], hf.at[b], hsem.at[b % 2]).wait()


def call_attend_gather(q, k, v, xf, wo, n):
    nb, sd, hid = xf.shape
    half = n // 4
    s = nb * sd
    bf, f32 = jnp.bfloat16, jnp.float32
    return pl.pallas_call(
        functools.partial(attend_gather, n),
        out_shape=jax.ShapeDtypeStruct((nb, sd, hid), bf),
        in_specs=[ANY] * 5,
        out_specs=ANY,
        scratch_shapes=[
            pltpu.VMEM((nb, n, sd, HEAD), bf),
            pltpu.VMEM(wo.shape, bf),
            pltpu.VMEM((s, HEAD), bf),
            pltpu.VMEM((s, HEAD), bf),
            pltpu.VMEM((s, HEAD), bf),
            pltpu.VMEM((2, sd, hid), bf),
            pltpu.VMEM((2, sd, hid), bf),
            pltpu.VMEM((sd, HEAD), f32),
            pltpu.VMEM((sd, HEAD), f32),
            pltpu.VMEM((sd, HEAD), f32),
        ]
        + [DMA((half, nb))] * 4
        + [DMA((2 * half + 1, nb))] * 2
        + [DMA((4,)), DMA((2,)), DMA((2,))],
        compiler_params=pltpu.CompilerParams(collective_id=2, has_side_effects=True, vmem_limit_bytes=VMEM_BYTES),
        name="attend_gather",
    )(q, k, v, xf, wo)


def dispatch(cap, per, meta, hf, h_own, buf):
    s = pl.program_id(0)
    me = lax.axis_index("sp")
    sd = hf.shape[1]
    kp = meta.shape[1] // 2
    chosen, gates = meta[0, :kp, :], meta[0, kp:, :]
    mine, gate = [], []
    for j in range(per):
        hit = chosen == (me * per + j).astype(jnp.float32)
        mine.append(jnp.max(jnp.where(hit, 1.0, 0.0), axis=0, keepdims=True))
        gate.append(jnp.sum(jnp.where(hit, gates, 0.0), axis=0, keepdims=True))
    low = lax.broadcasted_iota(jnp.int32, (sd, sd), 0) < lax.broadcasted_iota(jnp.int32, (sd, sd), 1)
    every = jnp.concatenate(mine + [jnp.zeros((8 - per, sd), jnp.float32)], axis=0).astype(jnp.bfloat16)
    rank = jnp.dot(every, jnp.where(low, 1.0, 0.0).astype(jnp.bfloat16), preferred_element_type=jnp.float32)
    place = lax.broadcasted_iota(jnp.int32, (cap, sd), 0).astype(jnp.float32)
    picks, ws = [], []
    for j in range(per):
        at = jnp.where(mine[j] > 0.5, rank[j : j + 1, :], -1.0) == place
        picks.append(jnp.where(at, 1.0, 0.0))
        ws.append(jnp.sum(jnp.where(at, gate[j], 0.0), axis=1, keepdims=True))
    pick = jnp.concatenate(picks, axis=0).astype(jnp.bfloat16)
    w = jnp.concatenate(ws, axis=0)
    hid = hf.shape[2]
    tile = 512
    for t in range(hid // tile):
        cols = pl.ds(t * tile, tile)
        rows = w * jnp.dot(pick, hf[0, :, cols], preferred_element_type=jnp.float32)
        for j in range(per):
            buf[j, :, cols] = rows[j * cap : (j + 1) * cap, :].astype(jnp.bfloat16)

    @pl.when(s == me)
    def _():
        h_own[...] = hf[0]


def call_dispatch(meta, hf, cap, per):
    n, sd, hid = hf.shape
    return pl.pallas_call(
        functools.partial(dispatch, cap, per),
        grid=(n,),
        out_shape=(jax.ShapeDtypeStruct((sd, hid), jnp.bfloat16), jax.ShapeDtypeStruct((per, n * cap, hid), jnp.bfloat16)),
        in_specs=[pl.BlockSpec((1,) + meta.shape[1:], lambda s: (s, 0, 0)), pl.BlockSpec((1, sd, hid), lambda s: (s, 0, 0))],
        out_specs=(pl.BlockSpec((sd, hid), lambda s: (0, 0)), pl.BlockSpec((per, cap, hid), lambda s: (0, s, 0))),
        compiler_params=pltpu.CompilerParams(dimension_semantics=("arbitrary",), vmem_limit_bytes=48 * 1024 * 1024),
        name="dispatch",
    )(meta, hf)


def routing(idx, probs):
    top = idx.shape[1]
    pad = -top % 8
    hot = idx[:, :, None] == jnp.arange(probs.shape[1])[None, None, :]
    sel = jnp.sum(jnp.where(hot, probs[:, None, :], 0.0), axis=2)
    w = sel / jnp.sum(sel, axis=1, keepdims=True)
    e = jnp.pad(idx.astype(jnp.float32), ((0, 0), (0, pad)), constant_values=-1.0)
    return jnp.concatenate([e, jnp.pad(w, ((0, 0), (0, pad)))], axis=1).T


def solution(mesh):
    n = mesh.shape["sp"]
    row = P(("dp", "sp"), None)
    full = P(None, None)

    def local(x, wq, wk, wv, wo, idx, probs):
        sd, hid = x.shape
        ne = probs.shape[1]
        cap = 2 * sd * idx.shape[1] // ne
        inv = ROPE_BASE ** (-jnp.arange(HEAD // 2, dtype=jnp.float32) * (2.0 / HEAD))
        inv = jnp.concatenate([inv, inv])[None, :]
        meta = routing(idx, probs)
        xf, q, k, v, metas = call_gather_project(x, wq, wk, wv, inv, meta, n)
        q, k, v = (a.reshape(n * sd, HEAD) for a in (q, k, v))
        hf = call_attend_gather(q, k, v, xf, wo, n)
        h, buf = call_dispatch(metas, hf, cap, ne // n)
        return h, buf

    return jax.shard_map(local, mesh=mesh, in_specs=(row, full, full, full, full, row, row), out_specs=(row, P(("dp", "sp"), None, None)), check_vma=False)
```

```python
import functools
import math
import jax
import jax.numpy as jnp
from jax import lax
from jax.experimental import pallas as pl
from jax.experimental.pallas import tpu as pltpu
from jax.sharding import PartitionSpec as P

HEAD = 128
ROPE_BASE = 1000000.0
MESH = pl.DeviceIdType.MESH
ANY = pl.BlockSpec(memory_space=pl.ANY)
VM = pl.BlockSpec(memory_space=pltpu.VMEM)
DMA = pltpu.SemaphoreType.DMA
VMEM_BYTES = 64 * 1024 * 1024 - 64 * 1024


class Ring:
    def __init__(self, n):
        self.chips = n // 2
        self.half = self.chips // 2
        self.me = lax.axis_index("sp")
        self.z = self.me // 2
        self.c = self.me % 2
        self.right = self.at(1)
        self.left = self.at(-1)
        self.part = self.z * 2 + 1 - self.c

    def at(self, d, other=False):
        c = 1 - self.c if other else self.c
        return lax.rem(self.z + self.chips + d, self.chips) * 2 + c

    def barrier(self):
        bar = pltpu.get_barrier_semaphore()
        for dev in (self.right, self.left, self.part):
            pl.semaphore_signal(bar, inc=1, device_id={"sp": dev}, device_id_type=MESH)
        pl.semaphore_wait(bar, 3)


def remote(src, dst, ss, rs, dev):
    return pltpu.make_async_remote_copy(src_ref=src, dst_ref=dst, send_sem=ss, recv_sem=rs, device_id={"sp": dev}, device_id_type=MESH)


def gather_project(n, pieces, x, wq, wk, wv, inv, meta, xf, qo, ko, vo, mo, xs, wb, qs, ks, vs, ms, tb, cws, cwr, ccs, ccr, pts, ptr, wsem, osem):
    r = Ring(n)
    me, half = r.me, r.half
    sd, hid = x.shape
    rows = sd // pieces
    cols = pl.ds(pl.multiple_of(me * HEAD, HEAD), HEAD)
    own = [pltpu.make_async_copy(w.at[:, cols], wb.at[:, pl.ds(i * HEAD, HEAD)], wsem.at[i]) for i, w in enumerate((wq, wk, wv))]
    own.append(pltpu.make_async_copy(x, xs.at[me], wsem.at[3]))
    own.append(pltpu.make_async_copy(meta, ms.at[me], wsem.at[4]))
    for cp in own:
        cp.start()
    r.barrier()

    def blk(chunk, p):
        return ms.at[chunk] if p == pieces else xs.at[chunk, pl.ds(p * rows, rows)]

    def src(p):
        return meta if p == pieces else x.at[pl.ds(p * rows, rows)]

    sent = []

    def go(cp):
        cp.start()
        sent.append(cp)

    order = [pieces] + list(range(pieces))

    def takes(d, p, cw):
        if d < half:
            return True
        return d == half and (cw if p == pieces else (p < pieces // 2) == cw)

    for p in order:
        go(remote(src(p), blk(me, p), cws.at[0, p], cwr.at[0, p], r.right))
        go(remote(src(p), blk(me, p), ccs.at[0, p], ccr.at[0, p], r.left))
        go(remote(src(p), blk(me, p), pts.at[0, p], ptr.at[0, p], r.part))

    outs = []

    def out(src_, dst, i, slot):
        cp = pltpu.make_async_copy(src_, dst, osem.at[i, slot])
        cp.start()
        outs.append(cp)

    def table(chunk):
        pos = (chunk * sd + lax.broadcasted_iota(jnp.int32, (sd, HEAD), 0)).astype(jnp.float32)
        ang = pos * inv[...]
        si = jnp.sin(ang)
        return jnp.cos(ang), jnp.where(lax.broadcasted_iota(jnp.int32, (sd, HEAD), 1) < HEAD // 2, -si, si)

    def project(chunk, slot, rot=None):
        out(xs.at[chunk], xf.at[chunk], 0, slot)
        acc = jnp.dot(xs[chunk], wb[...], preferred_element_type=jnp.float32)
        co, si = table(chunk) if rot is None else (tb[rot, 0], tb[rot, 1])
        q = acc[:, :HEAD]
        k = acc[:, HEAD : 2 * HEAD]
        qs[chunk] = (q * co + pltpu.roll(q, HEAD // 2, 1) * si).astype(jnp.bfloat16)
        ks[chunk] = (k * co + pltpu.roll(k, HEAD // 2, 1) * si).astype(jnp.bfloat16)
        vs[chunk] = acc[:, 2 * HEAD :].T.astype(jnp.bfloat16)
        out(qs.at[chunk], qo.at[chunk], 1, slot)
        out(ks.at[chunk], ko.at[chunk], 2, slot)
        out(vs.at[chunk], vo.at[:, pl.ds(pl.multiple_of(chunk * sd, sd), sd)], 3, slot)

    def crossed(chunk, s):
        for p in order:
            remote(blk(chunk, p), blk(chunk, p), pts.at[s, p], ptr.at[s, p], r.part).wait_recv()

    for cp in own:
        cp.wait()
    project(me, 0)
    crossed(r.part, 0)
    project(r.part, 1)
    slot = 2
    for d in range(1, half + 1):
        a, b = r.at(-d), r.at(d)
        ao, bo = r.at(-d, True), r.at(d, True)
        s1 = 2 * d - 1
        s2 = 2 * d if d < half else s1
        if d == half:
            for i, chunk in enumerate((a, ao)):
                tb[i, 0], tb[i, 1] = table(chunk)
        for p in order:
            if takes(d, p, True):
                remote(blk(a, p), blk(a, p), cws.at[d - 1, p], cwr.at[d - 1, p], r.right).wait_recv()
                if takes(d + 1, p, True):
                    go(remote(blk(a, p), blk(a, p), cws.at[d, p], cwr.at[d, p], r.right))
                go(remote(blk(a, p), blk(a, p), pts.at[s1, p], ptr.at[s1, p], r.part))
            if takes(d, p, False):
                remote(blk(b, p), blk(b, p), ccs.at[d - 1, p], ccr.at[d - 1, p], r.left).wait_recv()
                if takes(d + 1, p, False):
                    go(remote(blk(b, p), blk(b, p), ccs.at[d, p], ccr.at[d, p], r.left))
                go(remote(blk(b, p), blk(b, p), pts.at[s2, p], ptr.at[s2, p], r.part))
        end = d == half
        project(a, slot, 0 if end else None)
        if not end:
            project(b, slot + 1)
        crossed(ao, s1)
        project(ao, slot + 2 - end, 1 if end else None)
        if not end:
            crossed(bo, s2)
            project(bo, slot + 3)
        slot += 4
    last = pltpu.make_async_copy(ms, mo, wsem.at[5])
    last.start()
    for cp in sent:
        cp.wait_send()
    for cp in outs:
        cp.wait()
    last.wait()


def call_gather_project(x, wq, wk, wv, inv, meta, n, pieces=4):
    sd, hid = x.shape
    half = n // 4
    bf = jnp.bfloat16
    head = jax.ShapeDtypeStruct((n, sd, HEAD), bf)
    return pl.pallas_call(
        functools.partial(gather_project, n, pieces),
        out_shape=(jax.ShapeDtypeStruct((n, sd, hid), bf), head, head, jax.ShapeDtypeStruct((HEAD, n * sd), bf), jax.ShapeDtypeStruct((n,) + meta.shape, meta.dtype)),
        in_specs=[ANY, ANY, ANY, ANY, VM, ANY],
        out_specs=(ANY,) * 5,
        scratch_shapes=[
            pltpu.VMEM((n, sd, hid), bf),
            pltpu.VMEM((hid, 3 * HEAD), bf),
            pltpu.VMEM((n, sd, HEAD), bf),
            pltpu.VMEM((n, sd, HEAD), bf),
            pltpu.VMEM((n, HEAD, sd), bf),
            pltpu.VMEM((n,) + meta.shape, meta.dtype),
            pltpu.VMEM((2, 2, sd, HEAD), jnp.float32),
        ]
        + [DMA((half, pieces + 1))] * 4
        + [DMA((2 * half, pieces + 1))] * 2
        + [DMA((6,)), DMA((4, n))],
        compiler_params=pltpu.CompilerParams(collective_id=1, has_side_effects=True, vmem_limit_bytes=VMEM_BYTES),
        name="gather_project",
    )(x, wq, wk, wv, inv, meta)


def attend_block(i, qT, kb, vT, m, l, acc, sa, sb, between):
    size = qT.shape[1]
    c = math.log2(math.e) / math.sqrt(HEAD)
    m[...] = jnp.full(m.shape, -jnp.inf, jnp.float32)
    l[...] = jnp.zeros(l.shape, jnp.float32)
    acc[...] = jnp.zeros(acc.shape, jnp.float32)

    def at(j):
        return pl.ds(pl.multiple_of(j * size, size), size)

    def score(j, ref):
        ref[...] = jnp.dot(kb[at(j), :], qT[...], preferred_element_type=jnp.float32)

    def soften(j, ref, masked):
        s = ref[...]
        if masked:
            kp = lax.broadcasted_iota(jnp.int32, (size, size), 0)
            qp = lax.broadcasted_iota(jnp.int32, (size, size), 1)
            s = jnp.where(kp <= qp, s, -jnp.inf)
        old = m[...]
        new = jnp.maximum(old, jnp.max(s, axis=0, keepdims=True))
        p = jnp.exp2(s * c - new * c)
        alpha = jnp.exp2((old - new) * c)
        l[...] = l[...] * alpha + jnp.sum(p, axis=0, keepdims=True)
        acc[...] = acc[...] * alpha + jnp.dot(vT[:, at(j)], p.astype(jnp.bfloat16), preferred_element_type=jnp.float32)
        m[...] = new

    score(0, sa)
    between()

    def body(jj, carry):
        score(2 * jj + 1, sb)
        soften(2 * jj, sa, False)
        score(2 * jj + 2, sa)
        soften(2 * jj + 1, sb, False)
        return carry

    lax.fori_loop(0, i // 2, body, 0)

    @pl.when(i % 2 == 1)
    def _():
        score(i, sb)
        soften(i - 1, sa, False)
        soften(i, sb, True)

    @pl.when(i % 2 == 0)
    def _():
        soften(i, sa, True)

    return (acc[...] / l[...]).T.astype(jnp.bfloat16)


def attend_gather(n, q, k, v, xf, wo, hf, o, wb, qb, kb, vb, xb, hb, qT, m, l, acc, sa, sb, cws, cwr, ccs, ccr, pts, ptr, gs, gr, lsem, xsem, hsem):
    r = Ring(n)
    me, half = r.me, r.half
    nb, _, bq, _ = o.shape
    hid = wo.shape[1]
    cut = bq // 2
    tile = 512
    load = [pltpu.make_async_copy(a, b, lsem.at[i]) for i, (a, b) in enumerate(((q, qb), (k, kb), (v, vb), (wo, wb)))]
    for cp in load:
        cp.start()
    pltpu.make_async_copy(xf.at[r.c], xb.at[0], xsem.at[0]).start()
    r.barrier()
    for cp in load[:3]:
        cp.wait()

    lo, hi, whole = pl.ds(0, cut), pl.ds(cut, cut), pl.ds(0, bq)

    def cw(b, d):
        chunk = r.at(-d)
        ref = o.at[b, chunk, lo if d + 1 == half else whole]
        return remote(ref, ref, cws.at[d, b], cwr.at[d, b], r.right)

    def ccw(b, d):
        chunk = r.at(d)
        ref = o.at[b, chunk, hi if d + 1 == half else whole]
        return remote(ref, ref, ccs.at[d, b], ccr.at[d, b], r.left)

    def cw_in(b, d):
        ref = o.at[b, r.at(-d), lo if d == half else whole]
        return remote(ref, ref, cws.at[d - 1, b], cwr.at[d - 1, b], r.right)

    def ccw_in(b, d):
        ref = o.at[b, r.at(d), hi if d == half else whole]
        return remote(ref, ref, ccs.at[d - 1, b], ccr.at[d - 1, b], r.left)

    def cross(b, s, other):
        d = (s + 1) // 2
        sign = -1 if s % 2 == 1 else 1
        rows = whole if d < half else (lo if sign < 0 else hi)
        ref = o.at[b, r.at(sign * d, other), rows]
        return remote(ref, ref, pts.at[s, b], ptr.at[s, b], r.part)

    def mine(b):
        return b % 2 == r.c

    def give(b, s):
        pl.when(b % 2 != r.c)(lambda: cross(b, s, False).start())

    def send(b):
        cw(b, 0).start()
        ccw(b, 0).start()
        give(b, 0)

    def serve(b, d):
        cw_in(b, d).wait_recv()
        if d < half:
            cw(b, d).start()
        give(b, 2 * d - 1)
        ccw_in(b, d).wait_recv()
        if d < half:
            ccw(b, d).start()
        give(b, 2 * d)

    pairs = nb // 2
    ahead = 2
    last = 2 * half - 3

    def attend(i, carry):
        qT[...] = qb[pl.ds(pl.multiple_of(i * 2 * bq, 2 * bq), 2 * bq), :].T

        def between():
            @pl.when(i > 0)
            def _():
                send(2 * i - 2)
                send(2 * i - 1)

            @pl.when(i == pairs - 1)
            def _():
                for b in range(ahead):
                    serve(b, 1)

        out = attend_block(i, qT, kb, vb, m, l, acc, sa, sb, between)
        o[2 * i, me] = out[:bq]
        o[2 * i + 1, me] = out[bq:]
        return carry

    def store(b):
        i = b // 2 % 2
        return pltpu.make_async_copy(hb.at[i], hf.at[b], hsem.at[i])

    def share(b):
        i = b // 2 % 2
        return remote(hb.at[i], hf.at[b], gs.at[b // 2], gr.at[b // 2], r.part)

    def fetch(b):
        i = b // 2 % 2
        return pltpu.make_async_copy(xf.at[b], xb.at[i], xsem.at[i])

    def project(b):
        i = b // 2 % 2
        pl.when(b + 2 < nb)(lambda: fetch(b + 2).start())
        fetch(b).wait()

        @pl.when(b >= 4)
        def _():
            store(b - 4).wait()
            share(b - 4).wait_send()

        def cols(t, carry):
            at = pl.ds(pl.multiple_of(t * tile, tile), tile)
            lhs = jnp.concatenate([o[b, j] for j in range(n)], axis=1)
            y = jnp.dot(lhs, wb[:, at], preferred_element_type=jnp.float32)
            hb[i, :, at] = (xb[i, :, at].astype(jnp.float32) + y).astype(jnp.bfloat16)
            return carry

        lax.fori_loop(0, hid // tile, cols, 0)
        store(b).start()
        share(b).start()

    lax.fori_loop(0, pairs, attend, 0)
    load[3].wait()
    send(nb - 2)
    send(nb - 1)

    def when_in(b, f):
        pl.when(jnp.logical_and(b >= 0, b < nb))(f)

    def step(i, carry):
        for d in range(2, half):
            when_in(i + 4 - 2 * d, lambda d=d: serve(i + 4 - 2 * d, d))
        when_in(i + ahead, lambda: serve(i + ahead, 1))
        when_in(i - last + 1, lambda: serve(i - last + 1, half))
        b = i - last

        @pl.when(jnp.logical_and(b >= 0, mine(b)))
        def _():
            for s in range(2 * half + 1):
                cross(b, s, True).wait_recv()
            project(b)

        return carry

    lax.fori_loop(0, nb + last, step, 0)

    def drain(b, carry):
        for d in range(half):
            cw(b, d).wait_send()
            ccw(b, d).wait_send()

        @pl.when(mine(b))
        def _():
            pl.when(b >= nb - 4)(lambda: (store(b).wait(), share(b).wait_send()) and None)

        @pl.when(jnp.logical_not(mine(b)))
        def _():
            for s in range(2 * half + 1):
                cross(b, s, False).wait_send()
            share(b).wait_recv()

        return carry

    lax.fori_loop(0, nb, drain, 0)


def call_attend_gather(q, k, v, xf, wo, n):
    nb, sd, hid = xf.shape
    half = n // 4
    s = nb * sd
    bf, f32 = jnp.bfloat16, jnp.float32
    return pl.pallas_call(
        functools.partial(attend_gather, n),
        out_shape=jax.ShapeDtypeStruct((nb, sd, hid), bf),
        in_specs=[ANY] * 5,
        out_specs=ANY,
        scratch_shapes=[
            pltpu.VMEM((nb, n, sd, HEAD), bf),
            pltpu.VMEM(wo.shape, bf),
            pltpu.VMEM((s, HEAD), bf),
            pltpu.VMEM((s, HEAD), bf),
            pltpu.VMEM((HEAD, s), bf),
            pltpu.VMEM((2, sd, hid), bf),
            pltpu.VMEM((2, sd, hid), bf),
            pltpu.VMEM((HEAD, 2 * sd), bf),
            pltpu.VMEM((1, 2 * sd), f32),
            pltpu.VMEM((1, 2 * sd), f32),
            pltpu.VMEM((HEAD, 2 * sd), f32),
            pltpu.VMEM((2 * sd, 2 * sd), f32),
            pltpu.VMEM((2 * sd, 2 * sd), f32),
        ]
        + [DMA((half, nb))] * 4
        + [DMA((2 * half + 1, nb))] * 2
        + [DMA((nb // 2,))] * 2
        + [DMA((4,)), DMA((2,)), DMA((2,))],
        compiler_params=pltpu.CompilerParams(collective_id=2, has_side_effects=True, vmem_limit_bytes=VMEM_BYTES),
        name="attend_gather",
    )(q, k, v, xf, wo)


def dispatch(cap, per, meta, hf, h_own, buf, low):
    s = pl.program_id(0)
    me = lax.axis_index("sp")
    group, sd, hid = hf.shape
    kp = meta.shape[1] // 2

    @pl.when(s == 0)
    def _():
        earlier = lax.broadcasted_iota(jnp.int32, (sd, sd), 0) < lax.broadcasted_iota(jnp.int32, (sd, sd), 1)
        low[...] = jnp.where(earlier, 1.0, 0.0).astype(jnp.bfloat16)

    mine, gate = [], []
    for i in range(group):
        chosen, gates = meta[i, :kp, :], meta[i, kp:, :]
        for j in range(per):
            hit = chosen == (me * per + j).astype(jnp.float32)
            mine.append(jnp.max(jnp.where(hit, 1.0, 0.0), axis=0, keepdims=True))
            gate.append(jnp.sum(jnp.where(hit, gates, 0.0), axis=0, keepdims=True))
    every = jnp.concatenate(mine, axis=0)
    rank = jnp.dot(every.astype(jnp.bfloat16), low[...], preferred_element_type=jnp.float32)
    rank = jnp.where(every > 0.5, rank, -1.0)
    place = lax.broadcasted_iota(jnp.int32, (cap, sd), 0).astype(jnp.float32)
    tile = 512
    pick, w = [], []
    for i in range(group):
        picks, ws = [], []
        for j in range(per):
            at = rank[i * per + j : i * per + j + 1, :] == place
            picks.append(jnp.where(at, 1.0, 0.0))
            ws.append(jnp.sum(jnp.where(at, gate[i * per + j], 0.0), axis=1, keepdims=True))
        pick.append(jnp.concatenate(picks, axis=0).astype(jnp.bfloat16))
        w.append(jnp.concatenate(ws, axis=0))
    for t in range(hid // tile):
        cols = pl.ds(t * tile, tile)
        rows = [w[i] * jnp.dot(pick[i], hf[i, :, cols], preferred_element_type=jnp.float32) for i in range(group)]
        for j in range(per):
            buf[j, :, cols] = jnp.concatenate([y[j * cap : (j + 1) * cap] for y in rows], axis=0).astype(jnp.bfloat16)

    @pl.when(s == me // group)
    def _():
        h_own[...] = hf[me % group]


def call_dispatch(meta, hf, cap, per, group=2):
    n, sd, hid = hf.shape
    return pl.pallas_call(
        functools.partial(dispatch, cap, per),
        grid=(n // group,),
        out_shape=(jax.ShapeDtypeStruct((sd, hid), jnp.bfloat16), jax.ShapeDtypeStruct((per, n * cap, hid), jnp.bfloat16)),
        in_specs=[pl.BlockSpec((group,) + meta.shape[1:], lambda s: (s, 0, 0)), pl.BlockSpec((group, sd, hid), lambda s: (s, 0, 0))],
        out_specs=(pl.BlockSpec((sd, hid), lambda s: (0, 0)), pl.BlockSpec((per, group * cap, hid), lambda s: (0, s, 0))),
        scratch_shapes=[pltpu.VMEM((sd, sd), jnp.bfloat16)],
        compiler_params=pltpu.CompilerParams(dimension_semantics=("arbitrary",), vmem_limit_bytes=48 * 1024 * 1024),
        name="dispatch",
    )(meta, hf)


def routing(idx, probs):
    top = idx.shape[1]
    pad = -top % 8
    hot = idx[:, :, None] == jnp.arange(probs.shape[1])[None, None, :]
    sel = jnp.sum(jnp.where(hot, probs[:, None, :], 0.0), axis=2)
    w = sel / jnp.sum(sel, axis=1, keepdims=True)
    e = jnp.pad(idx.astype(jnp.float32), ((0, 0), (0, pad)), constant_values=-1.0)
    return jnp.concatenate([e, jnp.pad(w, ((0, 0), (0, pad)))], axis=1).T


def solution(mesh):
    n = mesh.shape["sp"]
    row = P(("dp", "sp"), None)
    full = P(None, None)

    def local(x, wq, wk, wv, wo, idx, probs):
        sd, hid = x.shape
        ne = probs.shape[1]
        cap = 2 * sd * idx.shape[1] // ne
        inv = ROPE_BASE ** (-jnp.arange(HEAD // 2, dtype=jnp.float32) * (2.0 / HEAD))
        inv = jnp.concatenate([inv, inv])[None, :]
        meta = routing(idx, probs)
        xf, q, k, v, metas = call_gather_project(x, wq, wk, wv, inv, meta, n)
        q, k = (a.reshape(n * sd, HEAD) for a in (q, k))
        hf = call_attend_gather(q, k, v, xf, wo, n)
        h, buf = call_dispatch(metas, hf, cap, ne // n)
        return h, buf

    return jax.shard_map(local, mesh=mesh, in_specs=(row, full, full, full, full, row, row), out_specs=(row, P(("dp", "sp"), None, None)), check_vma=False)
```

```python
import functools
import math
import jax
import jax.numpy as jnp
import numpy as np
from jax import lax
from jax.experimental import pallas as pl
from jax.experimental.pallas import tpu as pltpu
from jax.sharding import PartitionSpec as P

HEAD = 128
ROPE_BASE = 1000000.0
MESH = pl.DeviceIdType.MESH
ANY = pl.BlockSpec(memory_space=pl.ANY)
VM = pl.BlockSpec(memory_space=pltpu.VMEM)
DMA = pltpu.SemaphoreType.DMA
VMEM_BYTES = 64 * 1024 * 1024 - 64 * 1024


class Ring:
    def __init__(self, n):
        self.chips = n // 2
        self.half = self.chips // 2
        self.me = lax.axis_index("sp")
        self.z = self.me // 2
        self.c = self.me % 2
        self.right = self.at(1)
        self.left = self.at(-1)
        self.part = self.z * 2 + 1 - self.c

    def at(self, d, other=False):
        c = 1 - self.c if other else self.c
        return lax.rem(self.z + self.chips + d, self.chips) * 2 + c

    def barrier(self):
        bar = pltpu.get_barrier_semaphore()
        for dev in (self.right, self.left, self.part):
            pl.semaphore_signal(bar, inc=1, device_id={"sp": dev}, device_id_type=MESH)
        pl.semaphore_wait(bar, 3)


def remote(src, dst, ss, rs, dev):
    return pltpu.make_async_remote_copy(src_ref=src, dst_ref=dst, send_sem=ss, recv_sem=rs, device_id={"sp": dev}, device_id_type=MESH)


def gather_project(n, pieces, x, wq, wk, wv, inv, meta, xf, qo, ko, vo, mo, xs, wb, qs, ks, vs, ms, tb, cws, cwr, ccs, ccr, pts, ptr, wsem, osem):
    r = Ring(n)
    me, half = r.me, r.half
    sd, hid = x.shape
    rows = sd // pieces
    cols = pl.ds(pl.multiple_of(me * HEAD, HEAD), HEAD)
    own = [pltpu.make_async_copy(w.at[:, cols], wb.at[:, pl.ds(i * HEAD, HEAD)], wsem.at[i]) for i, w in enumerate((wq, wk, wv))]
    own.append(pltpu.make_async_copy(x, xs.at[me], wsem.at[3]))
    own.append(pltpu.make_async_copy(meta, ms.at[me], wsem.at[4]))
    for cp in own:
        cp.start()
    r.barrier()

    def blk(chunk, p):
        return ms.at[chunk] if p == pieces else xs.at[chunk, pl.ds(p * rows, rows)]

    def src(p):
        return meta if p == pieces else x.at[pl.ds(p * rows, rows)]

    sent = []

    def go(cp):
        cp.start()
        sent.append(cp)

    order = [pieces] + list(range(pieces))

    def takes(d, p, cw):
        if d < half:
            return True
        return d == half and (cw if p == pieces else (p < pieces // 2) == cw)

    for p in order:
        go(remote(src(p), blk(me, p), cws.at[0, p], cwr.at[0, p], r.right))
        go(remote(src(p), blk(me, p), ccs.at[0, p], ccr.at[0, p], r.left))
        go(remote(src(p), blk(me, p), pts.at[0, p], ptr.at[0, p], r.part))

    outs = []

    def out(src_, dst, i, slot):
        cp = pltpu.make_async_copy(src_, dst, osem.at[i, slot])
        cp.start()
        outs.append(cp)

    def table(chunk):
        pos = (chunk * sd + lax.broadcasted_iota(jnp.int32, (sd, HEAD), 0)).astype(jnp.float32)
        ang = pos * inv[...]
        si = jnp.sin(ang)
        return jnp.cos(ang), jnp.where(lax.broadcasted_iota(jnp.int32, (sd, HEAD), 1) < HEAD // 2, -si, si)

    def project(chunk, slot, rot=None):
        out(xs.at[chunk], xf.at[chunk], 0, slot)
        acc = jnp.dot(xs[chunk], wb[...], preferred_element_type=jnp.float32)
        co, si = table(chunk) if rot is None else (tb[rot, 0], tb[rot, 1])
        q = acc[:, :HEAD]
        k = acc[:, HEAD : 2 * HEAD]
        qs[chunk] = (q * co + pltpu.roll(q, HEAD // 2, 1) * si).astype(jnp.bfloat16)
        ks[chunk] = (k * co + pltpu.roll(k, HEAD // 2, 1) * si).astype(jnp.bfloat16)
        vs[chunk] = acc[:, 2 * HEAD :].T.astype(jnp.bfloat16)
        out(qs.at[chunk], qo.at[chunk], 1, slot)
        out(ks.at[chunk], ko.at[chunk], 2, slot)
        out(vs.at[chunk], vo.at[:, pl.ds(pl.multiple_of(chunk * sd, sd), sd)], 3, slot)

    def crossed(chunk, s):
        for p in order:
            remote(blk(chunk, p), blk(chunk, p), pts.at[s, p], ptr.at[s, p], r.part).wait_recv()

    for cp in own:
        cp.wait()
    project(me, 0)
    crossed(r.part, 0)
    project(r.part, 1)
    slot = 2
    for d in range(1, half + 1):
        a, b = r.at(-d), r.at(d)
        ao, bo = r.at(-d, True), r.at(d, True)
        s1 = 2 * d - 1
        s2 = 2 * d if d < half else s1
        if d == half:
            for i, chunk in enumerate((a, ao)):
                tb[i, 0], tb[i, 1] = table(chunk)
        for p in order:
            if takes(d, p, True):
                remote(blk(a, p), blk(a, p), cws.at[d - 1, p], cwr.at[d - 1, p], r.right).wait_recv()
                if takes(d + 1, p, True):
                    go(remote(blk(a, p), blk(a, p), cws.at[d, p], cwr.at[d, p], r.right))
                go(remote(blk(a, p), blk(a, p), pts.at[s1, p], ptr.at[s1, p], r.part))
            if takes(d, p, False):
                remote(blk(b, p), blk(b, p), ccs.at[d - 1, p], ccr.at[d - 1, p], r.left).wait_recv()
                if takes(d + 1, p, False):
                    go(remote(blk(b, p), blk(b, p), ccs.at[d, p], ccr.at[d, p], r.left))
                go(remote(blk(b, p), blk(b, p), pts.at[s2, p], ptr.at[s2, p], r.part))
        end = d == half
        project(a, slot, 0 if end else None)
        if not end:
            project(b, slot + 1)
        crossed(ao, s1)
        project(ao, slot + 2 - end, 1 if end else None)
        if not end:
            crossed(bo, s2)
            project(bo, slot + 3)
        slot += 4
    last = pltpu.make_async_copy(ms, mo, wsem.at[5])
    last.start()
    for cp in sent:
        cp.wait_send()
    for cp in outs:
        cp.wait()
    last.wait()


def call_gather_project(x, wq, wk, wv, inv, meta, n, pieces=4):
    sd, hid = x.shape
    half = n // 4
    bf = jnp.bfloat16
    head = jax.ShapeDtypeStruct((n, sd, HEAD), bf)
    return pl.pallas_call(
        functools.partial(gather_project, n, pieces),
        out_shape=(jax.ShapeDtypeStruct((n, sd, hid), bf), head, head, jax.ShapeDtypeStruct((HEAD, n * sd), bf), jax.ShapeDtypeStruct((n,) + meta.shape, meta.dtype)),
        in_specs=[ANY, ANY, ANY, ANY, VM, ANY],
        out_specs=(ANY,) * 5,
        scratch_shapes=[
            pltpu.VMEM((n, sd, hid), bf),
            pltpu.VMEM((hid, 3 * HEAD), bf),
            pltpu.VMEM((n, sd, HEAD), bf),
            pltpu.VMEM((n, sd, HEAD), bf),
            pltpu.VMEM((n, HEAD, sd), bf),
            pltpu.VMEM((n,) + meta.shape, meta.dtype),
            pltpu.VMEM((2, 2, sd, HEAD), jnp.float32),
        ]
        + [DMA((half, pieces + 1))] * 4
        + [DMA((2 * half, pieces + 1))] * 2
        + [DMA((6,)), DMA((4, n))],
        compiler_params=pltpu.CompilerParams(collective_id=1, has_side_effects=True, vmem_limit_bytes=VMEM_BYTES),
        name="gather_project",
    )(x, wq, wk, wv, inv, meta)


def attend_block(i, qT, kb, vT, m, l, acc, sa, sb, between):
    size = qT.shape[1]
    c = math.log2(math.e) / math.sqrt(HEAD)
    m[...] = jnp.full(m.shape, -jnp.inf, jnp.float32)
    l[...] = jnp.zeros(l.shape, jnp.float32)
    acc[...] = jnp.zeros(acc.shape, jnp.float32)

    def at(j):
        return pl.ds(pl.multiple_of(j * size, size), size)

    def score(j, ref):
        ref[...] = jnp.dot(kb[at(j), :], qT[...], preferred_element_type=jnp.float32)

    def soften(j, ref, masked):
        s = ref[...]
        if masked:
            kp = lax.broadcasted_iota(jnp.int32, (size, size), 0)
            qp = lax.broadcasted_iota(jnp.int32, (size, size), 1)
            s = jnp.where(kp <= qp, s, -jnp.inf)
        old = m[...]
        new = jnp.maximum(old, jnp.max(s, axis=0, keepdims=True))
        p = jnp.exp2(s * c - new * c)
        alpha = jnp.exp2((old - new) * c)
        l[...] = l[...] * alpha + jnp.sum(p, axis=0, keepdims=True)
        acc[...] = acc[...] * alpha + jnp.dot(vT[:, at(j)], p.astype(jnp.bfloat16), preferred_element_type=jnp.float32)
        m[...] = new

    score(0, sa)
    between()

    def body(jj, carry):
        score(2 * jj + 1, sb)
        soften(2 * jj, sa, False)
        score(2 * jj + 2, sa)
        soften(2 * jj + 1, sb, False)
        return carry

    lax.fori_loop(0, i // 2, body, 0)

    @pl.when(i % 2 == 1)
    def _():
        score(i, sb)
        soften(i - 1, sa, False)
        soften(i, sb, True)

    @pl.when(i % 2 == 0)
    def _():
        soften(i, sa, True)

    return (acc[...] / l[...]).T.astype(jnp.bfloat16)


def attend_gather(n, q, k, v, xf, wo, hf, o, wb, qb, kb, vb, xb, hb, qT, m, l, acc, sa, sb, cws, cwr, ccs, ccr, pts, ptr, gs, gr, lsem, xsem, hsem):
    r = Ring(n)
    me, half = r.me, r.half
    nb, _, bq, _ = o.shape
    hid = wo.shape[1]
    cut = bq // 2
    width = hid // 2
    tile = 512
    tiles = width // tile
    half_cols = pl.ds(pl.multiple_of(r.c * width, width), width)
    load = [pltpu.make_async_copy(a, b, lsem.at[i]) for i, (a, b) in enumerate(((q, qb), (k, kb), (v, vb), (wo.at[:, half_cols], wb)))]
    for cp in load:
        cp.start()
    pltpu.make_async_copy(xf.at[0, :, half_cols], xb.at[0], xsem.at[0]).start()
    r.barrier()
    for cp in load[:3]:
        cp.wait()

    lo, hi, whole = pl.ds(0, cut), pl.ds(cut, cut), pl.ds(0, bq)

    def cw(b, d):
        chunk = r.at(-d)
        ref = o.at[b, chunk, lo if d + 1 == half else whole]
        return remote(ref, ref, cws.at[d, b], cwr.at[d, b], r.right)

    def ccw(b, d):
        chunk = r.at(d)
        ref = o.at[b, chunk, hi if d + 1 == half else whole]
        return remote(ref, ref, ccs.at[d, b], ccr.at[d, b], r.left)

    def cw_in(b, d):
        ref = o.at[b, r.at(-d), lo if d == half else whole]
        return remote(ref, ref, cws.at[d - 1, b], cwr.at[d - 1, b], r.right)

    def ccw_in(b, d):
        ref = o.at[b, r.at(d), hi if d == half else whole]
        return remote(ref, ref, ccs.at[d - 1, b], ccr.at[d - 1, b], r.left)

    def cross(b, s, other):
        d = (s + 1) // 2
        sign = -1 if s % 2 == 1 else 1
        rows = whole if d < half else (lo if sign < 0 else hi)
        ref = o.at[b, r.at(sign * d, other), rows]
        return remote(ref, ref, pts.at[s, b], ptr.at[s, b], r.part)

    def give(b, s):
        cross(b, s, False).start()

    def send(b):
        cw(b, 0).start()
        ccw(b, 0).start()
        give(b, 0)

    def serve(b, d):
        cw_in(b, d).wait_recv()
        if d < half:
            cw(b, d).start()
        give(b, 2 * d - 1)
        ccw_in(b, d).wait_recv()
        if d < half:
            ccw(b, d).start()
        give(b, 2 * d)

    pairs = nb // 2
    ahead = 2
    last = 2 * half - 3

    def attend(i, carry):
        qT[...] = qb[pl.ds(pl.multiple_of(i * 2 * bq, 2 * bq), 2 * bq), :].T

        def between():
            @pl.when(i > 0)
            def _():
                send(2 * i - 2)
                send(2 * i - 1)

            @pl.when(i == pairs - 1)
            def _():
                for b in range(ahead):
                    serve(b, 1)

        out = attend_block(i, qT, kb, vb, m, l, acc, sa, sb, between)
        o[2 * i, me] = out[:bq]
        o[2 * i + 1, me] = out[bq:]
        return carry

    def store(b):
        return pltpu.make_async_copy(hb.at[b % 2], hf.at[b, :, half_cols], hsem.at[b % 2])

    def share(b, t):
        to = pl.ds(pl.multiple_of(r.c * width + t * tile, tile), tile)
        return remote(hb.at[b % 2, :, pl.ds(pl.multiple_of(t * tile, tile), tile)], hf.at[b, :, to], gs.at[b, t], gr.at[b, t], r.part)

    def fetch(b):
        return pltpu.make_async_copy(xf.at[b, :, half_cols], xb.at[b % 2], xsem.at[b % 2])

    def project(b):
        i = b % 2
        pl.when(b + 1 < nb)(lambda: fetch(b + 1).start())
        fetch(b).wait()

        @pl.when(b >= 2)
        def _():
            store(b - 2).wait()
            for t in range(tiles):
                share(b - 2, t).wait_send()

        def cols(t, carry):
            at = pl.ds(pl.multiple_of(t * tile, tile), tile)
            lhs = jnp.concatenate([o[b, j] for j in range(n)], axis=1)
            y = jnp.dot(lhs, wb[:, at], preferred_element_type=jnp.float32)
            hb[i, :, at] = (xb[i, :, at].astype(jnp.float32) + y).astype(jnp.bfloat16)
            share(b, t).start()
            return carry

        lax.fori_loop(0, tiles, cols, 0)
        store(b).start()

    lax.fori_loop(0, pairs, attend, 0)
    load[3].wait()
    send(nb - 2)
    send(nb - 1)

    def when_in(b, f):
        pl.when(jnp.logical_and(b >= 0, b < nb))(f)

    def step(i, carry):
        for d in range(2, half):
            when_in(i + 4 - 2 * d, lambda d=d: serve(i + 4 - 2 * d, d))
        when_in(i + ahead, lambda: serve(i + ahead, 1))
        when_in(i - last + 1, lambda: serve(i - last + 1, half))
        b = i - last

        @pl.when(b >= 0)
        def _():
            for s in range(2 * half + 1):
                cross(b, s, True).wait_recv()
            project(b)

        return carry

    lax.fori_loop(0, nb + last, step, 0)

    def drain(b, carry):
        for d in range(half):
            cw(b, d).wait_send()
            ccw(b, d).wait_send()

        for s in range(2 * half + 1):
            cross(b, s, False).wait_send()
        for t in range(tiles):
            share(b, t).wait_recv()

        @pl.when(b >= nb - 2)
        def _():
            store(b).wait()
            for t in range(tiles):
                share(b, t).wait_send()

        return carry

    lax.fori_loop(0, nb, drain, 0)


def call_attend_gather(q, k, v, xf, wo, n):
    nb, sd, hid = xf.shape
    half = n // 4
    s = nb * sd
    bf, f32 = jnp.bfloat16, jnp.float32
    return pl.pallas_call(
        functools.partial(attend_gather, n),
        out_shape=jax.ShapeDtypeStruct((nb, sd, hid), bf),
        in_specs=[ANY] * 5,
        out_specs=ANY,
        scratch_shapes=[
            pltpu.VMEM((nb, n, sd, HEAD), bf),
            pltpu.VMEM((wo.shape[0], hid // 2), bf),
            pltpu.VMEM((s, HEAD), bf),
            pltpu.VMEM((s, HEAD), bf),
            pltpu.VMEM((HEAD, s), bf),
            pltpu.VMEM((2, sd, hid // 2), bf),
            pltpu.VMEM((2, sd, hid // 2), bf),
            pltpu.VMEM((HEAD, 2 * sd), bf),
            pltpu.VMEM((1, 2 * sd), f32),
            pltpu.VMEM((1, 2 * sd), f32),
            pltpu.VMEM((HEAD, 2 * sd), f32),
            pltpu.VMEM((2 * sd, 2 * sd), f32),
            pltpu.VMEM((2 * sd, 2 * sd), f32),
        ]
        + [DMA((half, nb))] * 4
        + [DMA((2 * half + 1, nb))] * 2
        + [DMA((nb, hid // 1024))] * 2
        + [DMA((4,)), DMA((2,)), DMA((2,))],
        compiler_params=pltpu.CompilerParams(collective_id=2, has_side_effects=True, vmem_limit_bytes=VMEM_BYTES),
        name="attend_gather",
    )(q, k, v, xf, wo)


def dispatch(cap, per, meta, hf, h_own, buf, hv, bv, low, isem, osem, hsem):
    me = lax.axis_index("sp")
    n, sd, hid = hf.shape
    kp = meta.shape[1] // 2
    tile = 512

    def fetch(s):
        return pltpu.make_async_copy(hf.at[s], hv.at[s], isem.at[s])

    def store(s, j):
        return pltpu.make_async_copy(bv.at[s, j], buf.at[j, pl.ds(pl.multiple_of(s * cap, 8), cap)], osem.at[s, j])

    for s in range(n):
        fetch(s).start()
    earlier = lax.broadcasted_iota(jnp.int32, (sd, sd), 0) < lax.broadcasted_iota(jnp.int32, (sd, sd), 1)
    low[...] = jnp.where(earlier, 1.0, 0.0).astype(jnp.bfloat16)
    place = lax.broadcasted_iota(jnp.int32, (cap, sd), 0).astype(jnp.float32)

    def source(s, carry):
        chosen, gates = meta[s, :kp, :], meta[s, kp:, :]
        mine, gate = [], []
        for j in range(per):
            hit = chosen == (me * per + j).astype(jnp.float32)
            mine.append(jnp.max(jnp.where(hit, 1.0, 0.0), axis=0, keepdims=True))
            gate.append(jnp.sum(jnp.where(hit, gates, 0.0), axis=0, keepdims=True))
        every = jnp.concatenate(mine + [jnp.zeros((8 - per, sd), jnp.float32)], axis=0)
        rank = jnp.dot(every.astype(jnp.bfloat16), low[...], preferred_element_type=jnp.float32)
        rank = jnp.where(every > 0.5, rank, -1.0)
        picks, ws = [], []
        for j in range(per):
            at = rank[j : j + 1, :] == place
            picks.append(jnp.where(at, 1.0, 0.0))
            ws.append(jnp.sum(jnp.where(at, gate[j], 0.0), axis=1, keepdims=True))
        pick = jnp.concatenate(picks, axis=0).astype(jnp.bfloat16)
        w = jnp.concatenate(ws, axis=0)
        fetch(s).wait()
        for t in range(hid // tile):
            cols = pl.ds(t * tile, tile)
            rows = w * jnp.dot(pick, hv[s, :, cols], preferred_element_type=jnp.float32)
            for j in range(per):
                bv[s, j, :, cols] = rows[j * cap : (j + 1) * cap, :].astype(jnp.bfloat16)
        for j in range(per):
            store(s, j).start()

        @pl.when(s == me)
        def _():
            pltpu.make_async_copy(hv.at[s], h_own, hsem).start()

        return carry

    lax.fori_loop(0, n, source, 0)

    def drain(s, carry):
        for j in range(per):
            store(s, j).wait()
        return carry

    lax.fori_loop(0, n, drain, 0)
    pltpu.make_async_copy(hv.at[me], h_own, hsem).wait()


def call_dispatch(meta, hf, cap, per):
    n, sd, hid = hf.shape
    return pl.pallas_call(
        functools.partial(dispatch, cap, per),
        out_shape=(jax.ShapeDtypeStruct((sd, hid), jnp.bfloat16), jax.ShapeDtypeStruct((per, n * cap, hid), jnp.bfloat16)),
        in_specs=[VM, ANY],
        out_specs=(ANY, ANY),
        scratch_shapes=[
            pltpu.VMEM((n, sd, hid), jnp.bfloat16),
            pltpu.VMEM((n, per, cap, hid), jnp.bfloat16),
            pltpu.VMEM((sd, sd), jnp.bfloat16),
            DMA((n,)),
            DMA((n, per)),
            DMA,
        ],
        compiler_params=pltpu.CompilerParams(vmem_limit_bytes=VMEM_BYTES),
        name="dispatch",
    )(meta, hf)


def routing(idx, probs):
    top = idx.shape[1]
    pad = -top % 8
    hot = idx[:, :, None] == jnp.arange(probs.shape[1])[None, None, :]
    sel = jnp.sum(jnp.where(hot, probs[:, None, :], 0.0), axis=2)
    w = sel / jnp.sum(sel, axis=1, keepdims=True)
    e = jnp.pad(idx.astype(jnp.float32), ((0, 0), (0, pad)), constant_values=-1.0)
    return jnp.concatenate([e, jnp.pad(w, ((0, 0), (0, pad)))], axis=1).T


def solution(mesh):
    n = mesh.shape["sp"]
    row = P(("dp", "sp"), None)
    full = P(None, None)

    def local(x, wq, wk, wv, wo, idx, probs):
        sd, hid = x.shape
        ne = probs.shape[1]
        cap = 2 * sd * idx.shape[1] // ne
        inv = jnp.asarray(np.tile(ROPE_BASE ** (-np.arange(HEAD // 2) * (2.0 / HEAD)), 2)[None, :], jnp.float32)
        meta = routing(idx, probs)
        xf, q, k, v, metas = call_gather_project(x, wq, wk, wv, inv, meta, n)
        q, k = (a.reshape(n * sd, HEAD) for a in (q, k))
        hf = call_attend_gather(q, k, v, xf, wo, n)
        h, buf = call_dispatch(metas, hf, cap, ne // n)
        return h, buf

    return jax.shard_map(local, mesh=mesh, in_specs=(row, full, full, full, full, row, row), out_specs=(row, P(("dp", "sp"), None, None)), check_vma=False)
```

```python
import functools
import math
import jax
import jax.numpy as jnp
import numpy as np
from jax import lax
from jax.experimental import pallas as pl
from jax.experimental.pallas import tpu as pltpu
from jax.sharding import PartitionSpec as P

HEAD = 128
ROPE_BASE = 1000000.0
MESH = pl.DeviceIdType.MESH
ANY = pl.BlockSpec(memory_space=pl.ANY)
VM = pl.BlockSpec(memory_space=pltpu.VMEM)
DMA = pltpu.SemaphoreType.DMA
VMEM_BYTES = 64 * 1024 * 1024 - 64 * 1024


class Ring:
    def __init__(self, n):
        self.chips = n // 2
        self.half = self.chips // 2
        self.me = lax.axis_index("sp")
        self.z = self.me // 2
        self.c = self.me % 2
        self.right = self.at(1)
        self.left = self.at(-1)
        self.part = self.z * 2 + 1 - self.c

    def at(self, d, other=False):
        c = 1 - self.c if other else self.c
        return lax.rem(self.z + self.chips + d, self.chips) * 2 + c

    def barrier(self):
        bar = pltpu.get_barrier_semaphore()
        for dev in (self.right, self.left, self.part):
            pl.semaphore_signal(bar, inc=1, device_id={"sp": dev}, device_id_type=MESH)
        pl.semaphore_wait(bar, 3)


def remote(src, dst, ss, rs, dev):
    return pltpu.make_async_remote_copy(src_ref=src, dst_ref=dst, send_sem=ss, recv_sem=rs, device_id={"sp": dev}, device_id_type=MESH)


def routing(idx, probs, half):
    top, sd = idx.shape
    expert = lax.broadcasted_iota(jnp.int32, probs.shape, 0)
    chosen = [idx[c : c + 1, :] for c in range(top)]
    sel = [jnp.sum(jnp.where(expert == e, probs[...], 0.0), axis=0, keepdims=True) for e in chosen]
    total = sum(sel[1:], sel[0])
    rows = [e.astype(jnp.float32) for e in chosen] + [jnp.full((half - top, sd), -1.0, jnp.float32)] * (half > top)
    rows += [w / total for w in sel] + [jnp.zeros((half - top, sd), jnp.float32)] * (half > top)
    return jnp.concatenate(rows, axis=0)


def gather_project(n, pieces, x, wq, wk, wv, inv, idx, probs, xf, qo, ko, vo, mo, xs, wb, qs, ks, vs, ms, tb, cws, cwr, ccs, ccr, pts, ptr, wsem, osem):
    r = Ring(n)
    me, half = r.me, r.half
    sd, hid = x.shape
    rows = sd // pieces
    cols = pl.ds(pl.multiple_of(me * HEAD, HEAD), HEAD)
    own = [pltpu.make_async_copy(w.at[:, cols], wb.at[:, pl.ds(i * HEAD, HEAD)], wsem.at[i]) for i, w in enumerate((wq, wk, wv))]
    own.append(pltpu.make_async_copy(x, xs.at[me], wsem.at[3]))
    for cp in own:
        cp.start()
    r.barrier()

    def blk(chunk, p):
        return ms.at[chunk] if p == pieces else xs.at[chunk, pl.ds(p * rows, rows)]

    def src(p):
        return ms.at[me] if p == pieces else x.at[pl.ds(p * rows, rows)]

    sent = []

    def go(cp):
        cp.start()
        sent.append(cp)

    order = list(range(pieces + 1))

    def takes(d, p, cw):
        if d < half:
            return True
        return d == half and (cw if p == pieces else (p < pieces // 2) == cw)

    def first(p):
        go(remote(src(p), blk(me, p), cws.at[0, p], cwr.at[0, p], r.right))
        go(remote(src(p), blk(me, p), ccs.at[0, p], ccr.at[0, p], r.left))
        go(remote(src(p), blk(me, p), pts.at[0, p], ptr.at[0, p], r.part))

    for p in range(pieces):
        first(p)
    ms[me] = routing(idx, probs, ms.shape[1] // 2)

    outs = []

    def out(src_, dst, i, slot):
        cp = pltpu.make_async_copy(src_, dst, osem.at[i, slot])
        cp.start()
        outs.append(cp)

    def table(chunk):
        pos = (chunk * sd + lax.broadcasted_iota(jnp.int32, (sd, HEAD), 0)).astype(jnp.float32)
        ang = pos * inv[...]
        si = jnp.sin(ang)
        return jnp.cos(ang), jnp.where(lax.broadcasted_iota(jnp.int32, (sd, HEAD), 1) < HEAD // 2, -si, si)

    def project(chunk, slot, rot=None):
        out(xs.at[chunk], xf.at[chunk], 0, slot)
        acc = jnp.dot(xs[chunk], wb[...], preferred_element_type=jnp.float32)
        co, si = table(chunk) if rot is None else (tb[rot, 0], tb[rot, 1])
        q = acc[:, :HEAD]
        k = acc[:, HEAD : 2 * HEAD]
        qs[chunk] = (q * co + pltpu.roll(q, HEAD // 2, 1) * si).astype(jnp.bfloat16)
        ks[chunk] = (k * co + pltpu.roll(k, HEAD // 2, 1) * si).astype(jnp.bfloat16)
        vs[chunk] = acc[:, 2 * HEAD :].T.astype(jnp.bfloat16)
        out(qs.at[chunk], qo.at[chunk], 1, slot)
        out(ks.at[chunk], ko.at[chunk], 2, slot)
        out(vs.at[chunk], vo.at[:, pl.ds(pl.multiple_of(chunk * sd, sd), sd)], 3, slot)

    def crossed(chunk, s):
        for p in order:
            remote(blk(chunk, p), blk(chunk, p), pts.at[s, p], ptr.at[s, p], r.part).wait_recv()

    for cp in own:
        cp.wait()
    project(me, 0)
    first(pieces)
    crossed(r.part, 0)
    project(r.part, 1)
    slot = 2
    for d in range(1, half + 1):
        a, b = r.at(-d), r.at(d)
        ao, bo = r.at(-d, True), r.at(d, True)
        s1 = 2 * d - 1
        s2 = 2 * d if d < half else s1
        if d == half:
            for i, chunk in enumerate((a, ao)):
                tb[i, 0], tb[i, 1] = table(chunk)
        for p in order:
            if takes(d, p, True):
                remote(blk(a, p), blk(a, p), cws.at[d - 1, p], cwr.at[d - 1, p], r.right).wait_recv()
                if takes(d + 1, p, True):
                    go(remote(blk(a, p), blk(a, p), cws.at[d, p], cwr.at[d, p], r.right))
                go(remote(blk(a, p), blk(a, p), pts.at[s1, p], ptr.at[s1, p], r.part))
            if takes(d, p, False):
                remote(blk(b, p), blk(b, p), ccs.at[d - 1, p], ccr.at[d - 1, p], r.left).wait_recv()
                if takes(d + 1, p, False):
                    go(remote(blk(b, p), blk(b, p), ccs.at[d, p], ccr.at[d, p], r.left))
                go(remote(blk(b, p), blk(b, p), pts.at[s2, p], ptr.at[s2, p], r.part))
        end = d == half
        project(a, slot, 0 if end else None)
        if not end:
            project(b, slot + 1)
        crossed(ao, s1)
        project(ao, slot + 2 - end, 1 if end else None)
        if not end:
            crossed(bo, s2)
            project(bo, slot + 3)
        slot += 4
    last = pltpu.make_async_copy(ms, mo, wsem.at[5])
    last.start()
    for cp in sent:
        cp.wait_send()
    for cp in outs:
        cp.wait()
    last.wait()


def call_gather_project(x, wq, wk, wv, inv, idx, probs, n, pieces=4):
    sd, hid = x.shape
    half = n // 4
    bf = jnp.bfloat16
    head = jax.ShapeDtypeStruct((n, sd, HEAD), bf)
    meta = jax.ShapeDtypeStruct((n, 2 * (idx.shape[0] + -idx.shape[0] % 8), sd), jnp.float32)
    return pl.pallas_call(
        functools.partial(gather_project, n, pieces),
        out_shape=(jax.ShapeDtypeStruct((n, sd, hid), bf), head, head, jax.ShapeDtypeStruct((HEAD, n * sd), bf), meta),
        in_specs=[ANY, ANY, ANY, ANY, VM, VM, VM],
        out_specs=(ANY,) * 5,
        scratch_shapes=[
            pltpu.VMEM((n, sd, hid), bf),
            pltpu.VMEM((hid, 3 * HEAD), bf),
            pltpu.VMEM((n, sd, HEAD), bf),
            pltpu.VMEM((n, sd, HEAD), bf),
            pltpu.VMEM((n, HEAD, sd), bf),
            pltpu.VMEM(meta.shape, meta.dtype),
            pltpu.VMEM((2, 2, sd, HEAD), jnp.float32),
        ]
        + [DMA((half, pieces + 1))] * 4
        + [DMA((2 * half, pieces + 1))] * 2
        + [DMA((6,)), DMA((4, n))],
        compiler_params=pltpu.CompilerParams(collective_id=1, has_side_effects=True, vmem_limit_bytes=VMEM_BYTES),
        name="gather_project",
    )(x, wq, wk, wv, inv, idx, probs)


def attend_block(i, qT, kb, vT, m, l, acc, sa, sb, between):
    size = qT.shape[1]
    c = math.log2(math.e) / math.sqrt(HEAD)
    m[...] = jnp.full(m.shape, -jnp.inf, jnp.float32)
    l[...] = jnp.zeros(l.shape, jnp.float32)
    acc[...] = jnp.zeros(acc.shape, jnp.float32)

    def at(j):
        return pl.ds(pl.multiple_of(j * size, size), size)

    def score(j, ref):
        ref[...] = jnp.dot(kb[at(j), :], qT[...], preferred_element_type=jnp.float32)

    def soften(j, ref, masked):
        s = ref[...]
        if masked:
            kp = lax.broadcasted_iota(jnp.int32, (size, size), 0)
            qp = lax.broadcasted_iota(jnp.int32, (size, size), 1)
            s = jnp.where(kp <= qp, s, -jnp.inf)
        old = m[...]
        new = jnp.maximum(old, jnp.max(s, axis=0, keepdims=True))
        p = jnp.exp2(s * c - new * c)
        alpha = jnp.exp2((old - new) * c)
        l[...] = l[...] * alpha + jnp.sum(p, axis=0, keepdims=True)
        acc[...] = acc[...] * alpha + jnp.dot(vT[:, at(j)], p.astype(jnp.bfloat16), preferred_element_type=jnp.float32)
        m[...] = new

    score(0, sa)
    between()

    def body(jj, carry):
        score(2 * jj + 1, sb)
        soften(2 * jj, sa, False)
        score(2 * jj + 2, sa)
        soften(2 * jj + 1, sb, False)
        return carry

    lax.fori_loop(0, i // 2, body, 0)

    @pl.when(i % 2 == 1)
    def _():
        score(i, sb)
        soften(i - 1, sa, False)
        soften(i, sb, True)

    @pl.when(i % 2 == 0)
    def _():
        soften(i, sa, True)

    return (acc[...] / l[...]).T.astype(jnp.bfloat16)


def attend_gather(n, q, k, v, xf, wo, hf, o, wb, qb, kb, vb, xb, hb, qT, m, l, acc, sa, sb, cws, cwr, ccs, ccr, pts, ptr, gs, gr, lsem, xsem, hsem):
    r = Ring(n)
    me, half = r.me, r.half
    nb, _, bq, _ = o.shape
    hid = wo.shape[1]
    cut = bq // 2
    width = hid // 2
    tile = 512
    tiles = width // tile
    half_cols = pl.ds(pl.multiple_of(r.c * width, width), width)
    head, tail = pl.ds(0, 2 * bq), pl.ds(2 * bq, (nb - 2) * bq)
    parts = [(a.at[rows], b.at[rows]) for rows in (head, tail) for a, b in ((q, qb), (k, kb))]
    parts[2:2] = [(v.at[:, head], vb.at[:, head])]
    parts += [(v.at[:, tail], vb.at[:, tail]), (wo.at[:, half_cols], wb)]
    load = [pltpu.make_async_copy(a, b, lsem.at[i]) for i, (a, b) in enumerate(parts)]
    for cp in load:
        cp.start()
    pltpu.make_async_copy(xf.at[0, :, half_cols], xb.at[0], xsem.at[0]).start()
    r.barrier()
    for cp in load[:3]:
        cp.wait()

    lo, hi, whole = pl.ds(0, cut), pl.ds(cut, cut), pl.ds(0, bq)

    def cw(b, d):
        chunk = r.at(-d)
        ref = o.at[b, chunk, lo if d + 1 == half else whole]
        return remote(ref, ref, cws.at[d, b], cwr.at[d, b], r.right)

    def ccw(b, d):
        chunk = r.at(d)
        ref = o.at[b, chunk, hi if d + 1 == half else whole]
        return remote(ref, ref, ccs.at[d, b], ccr.at[d, b], r.left)

    def cw_in(b, d):
        ref = o.at[b, r.at(-d), lo if d == half else whole]
        return remote(ref, ref, cws.at[d - 1, b], cwr.at[d - 1, b], r.right)

    def ccw_in(b, d):
        ref = o.at[b, r.at(d), hi if d == half else whole]
        return remote(ref, ref, ccs.at[d - 1, b], ccr.at[d - 1, b], r.left)

    def cross(b, s, other):
        d = (s + 1) // 2
        sign = -1 if s % 2 == 1 else 1
        rows = whole if d < half else (lo if sign < 0 else hi)
        ref = o.at[b, r.at(sign * d, other), rows]
        return remote(ref, ref, pts.at[s, b], ptr.at[s, b], r.part)

    def give(b, s):
        cross(b, s, False).start()

    def send(b):
        cw(b, 0).start()
        ccw(b, 0).start()
        give(b, 0)

    def serve(b, d):
        cw_in(b, d).wait_recv()
        if d < half:
            cw(b, d).start()
        give(b, 2 * d - 1)
        ccw_in(b, d).wait_recv()
        if d < half:
            ccw(b, d).start()
        give(b, 2 * d)

    pairs = nb // 2
    ahead = 2
    last = 2 * half - 3

    def attend(i, carry):
        @pl.when(i == 1)
        def _():
            for cp in load[3:6]:
                cp.wait()

        qT[...] = qb[pl.ds(pl.multiple_of(i * 2 * bq, 2 * bq), 2 * bq), :].T

        def between():
            @pl.when(i > 0)
            def _():
                send(2 * i - 2)
                send(2 * i - 1)

            @pl.when(i == pairs - 1)
            def _():
                for b in range(ahead):
                    serve(b, 1)

        out = attend_block(i, qT, kb, vb, m, l, acc, sa, sb, between)
        o[2 * i, me] = out[:bq]
        o[2 * i + 1, me] = out[bq:]
        return carry

    def store(b):
        return pltpu.make_async_copy(hb.at[b % 2], hf.at[b, :, half_cols], hsem.at[b % 2])

    def share(b, t):
        to = pl.ds(pl.multiple_of(r.c * width + t * tile, tile), tile)
        return remote(hb.at[b % 2, :, pl.ds(pl.multiple_of(t * tile, tile), tile)], hf.at[b, :, to], gs.at[b, t], gr.at[b, t], r.part)

    def fetch(b):
        return pltpu.make_async_copy(xf.at[b, :, half_cols], xb.at[b % 2], xsem.at[b % 2])

    def project(b):
        i = b % 2
        pl.when(b + 1 < nb)(lambda: fetch(b + 1).start())
        fetch(b).wait()

        @pl.when(b >= 2)
        def _():
            store(b - 2).wait()
            for t in range(tiles):
                share(b - 2, t).wait_send()

        def cols(t, carry):
            at = pl.ds(pl.multiple_of(t * tile, tile), tile)
            lhs = jnp.concatenate([o[b, j] for j in range(n)], axis=1)
            y = jnp.dot(lhs, wb[:, at], preferred_element_type=jnp.float32)
            hb[i, :, at] = (xb[i, :, at].astype(jnp.float32) + y).astype(jnp.bfloat16)
            share(b, t).start()
            return carry

        lax.fori_loop(0, tiles, cols, 0)
        store(b).start()

    lax.fori_loop(0, pairs, attend, 0)
    load[6].wait()
    send(nb - 2)
    send(nb - 1)

    def when_in(b, f):
        pl.when(jnp.logical_and(b >= 0, b < nb))(f)

    def step(i, carry):
        for d in range(2, half):
            when_in(i + 4 - 2 * d, lambda d=d: serve(i + 4 - 2 * d, d))
        when_in(i + ahead, lambda: serve(i + ahead, 1))
        when_in(i - last + 1, lambda: serve(i - last + 1, half))
        b = i - last

        @pl.when(b >= 0)
        def _():
            for s in range(2 * half + 1):
                cross(b, s, True).wait_recv()
            project(b)

        return carry

    lax.fori_loop(0, nb + last, step, 0)

    def drain(b, carry):
        for d in range(half):
            cw(b, d).wait_send()
            ccw(b, d).wait_send()

        for s in range(2 * half + 1):
            cross(b, s, False).wait_send()
        for t in range(tiles):
            share(b, t).wait_recv()

        @pl.when(b >= nb - 2)
        def _():
            store(b).wait()
            for t in range(tiles):
                share(b, t).wait_send()

        return carry

    lax.fori_loop(0, nb, drain, 0)


def call_attend_gather(q, k, v, xf, wo, n):
    nb, sd, hid = xf.shape
    half = n // 4
    s = nb * sd
    bf, f32 = jnp.bfloat16, jnp.float32
    return pl.pallas_call(
        functools.partial(attend_gather, n),
        out_shape=jax.ShapeDtypeStruct((nb, sd, hid), bf),
        in_specs=[ANY] * 5,
        out_specs=ANY,
        scratch_shapes=[
            pltpu.VMEM((nb, n, sd, HEAD), bf),
            pltpu.VMEM((wo.shape[0], hid // 2), bf),
            pltpu.VMEM((s, HEAD), bf),
            pltpu.VMEM((s, HEAD), bf),
            pltpu.VMEM((HEAD, s), bf),
            pltpu.VMEM((2, sd, hid // 2), bf),
            pltpu.VMEM((2, sd, hid // 2), bf),
            pltpu.VMEM((HEAD, 2 * sd), bf),
            pltpu.VMEM((1, 2 * sd), f32),
            pltpu.VMEM((1, 2 * sd), f32),
            pltpu.VMEM((HEAD, 2 * sd), f32),
            pltpu.VMEM((2 * sd, 2 * sd), f32),
            pltpu.VMEM((2 * sd, 2 * sd), f32),
        ]
        + [DMA((half, nb))] * 4
        + [DMA((2 * half + 1, nb))] * 2
        + [DMA((nb, hid // 1024))] * 2
        + [DMA((7,)), DMA((2,)), DMA((2,))],
        compiler_params=pltpu.CompilerParams(collective_id=2, has_side_effects=True, vmem_limit_bytes=VMEM_BYTES),
        name="attend_gather",
    )(q, k, v, xf, wo)


def dispatch(cap, per, meta, hf, h_own, buf, hv, bv, low, isem, osem, hsem):
    me = lax.axis_index("sp")
    n, sd, hid = hf.shape
    kp = meta.shape[1] // 2
    tile = 512

    def fetch(s):
        return pltpu.make_async_copy(hf.at[s], hv.at[s], isem.at[s])

    def store(s, j):
        return pltpu.make_async_copy(bv.at[s, j], buf.at[j, pl.ds(pl.multiple_of(s * cap, 8), cap)], osem.at[s, j])

    for s in range(n):
        fetch(s).start()
    earlier = lax.broadcasted_iota(jnp.int32, (sd, sd), 0) < lax.broadcasted_iota(jnp.int32, (sd, sd), 1)
    low[...] = jnp.where(earlier, 1.0, 0.0).astype(jnp.bfloat16)
    place = lax.broadcasted_iota(jnp.int32, (cap, sd), 0).astype(jnp.float32)

    def source(s, carry):
        chosen, gates = meta[s, :kp, :], meta[s, kp:, :]
        mine, gate = [], []
        for j in range(per):
            hit = chosen == (me * per + j).astype(jnp.float32)
            mine.append(jnp.max(jnp.where(hit, 1.0, 0.0), axis=0, keepdims=True))
            gate.append(jnp.sum(jnp.where(hit, gates, 0.0), axis=0, keepdims=True))
        every = jnp.concatenate(mine + [jnp.zeros((8 - per, sd), jnp.float32)], axis=0)
        rank = jnp.dot(every.astype(jnp.bfloat16), low[...], preferred_element_type=jnp.float32)
        rank = jnp.where(every > 0.5, rank, -1.0)
        picks, ws = [], []
        for j in range(per):
            at = rank[j : j + 1, :] == place
            picks.append(jnp.where(at, 1.0, 0.0))
            ws.append(jnp.sum(jnp.where(at, gate[j], 0.0), axis=1, keepdims=True))
        pick = jnp.concatenate(picks, axis=0).astype(jnp.bfloat16)
        w = jnp.concatenate(ws, axis=0)
        fetch(s).wait()
        for t in range(hid // tile):
            cols = pl.ds(t * tile, tile)
            rows = w * jnp.dot(pick, hv[s, :, cols], preferred_element_type=jnp.float32)
            for j in range(per):
                bv[s, j, :, cols] = rows[j * cap : (j + 1) * cap, :].astype(jnp.bfloat16)
        for j in range(per):
            store(s, j).start()

        @pl.when(s == me)
        def _():
            pltpu.make_async_copy(hv.at[s], h_own, hsem).start()

        return carry

    lax.fori_loop(0, n, source, 0)

    def drain(s, carry):
        for j in range(per):
            store(s, j).wait()
        return carry

    lax.fori_loop(0, n, drain, 0)
    pltpu.make_async_copy(hv.at[me], h_own, hsem).wait()


def call_dispatch(meta, hf, cap, per):
    n, sd, hid = hf.shape
    return pl.pallas_call(
        functools.partial(dispatch, cap, per),
        out_shape=(jax.ShapeDtypeStruct((sd, hid), jnp.bfloat16), jax.ShapeDtypeStruct((per, n * cap, hid), jnp.bfloat16)),
        in_specs=[VM, ANY],
        out_specs=(ANY, ANY),
        scratch_shapes=[
            pltpu.VMEM((n, sd, hid), jnp.bfloat16),
            pltpu.VMEM((n, per, cap, hid), jnp.bfloat16),
            pltpu.VMEM((sd, sd), jnp.bfloat16),
            DMA((n,)),
            DMA((n, per)),
            DMA,
        ],
        compiler_params=pltpu.CompilerParams(vmem_limit_bytes=VMEM_BYTES),
        name="dispatch",
    )(meta, hf)


def solution(mesh):
    n = mesh.shape["sp"]
    row = P(("dp", "sp"), None)
    full = P(None, None)

    def local(x, wq, wk, wv, wo, idx, probs):
        sd, hid = x.shape
        ne = probs.shape[1]
        cap = 2 * sd * idx.shape[1] // ne
        inv = jnp.asarray(np.tile(ROPE_BASE ** (-np.arange(HEAD // 2) * (2.0 / HEAD)), 2)[None, :], jnp.float32)
        xf, q, k, v, metas = call_gather_project(x, wq, wk, wv, inv, idx.T, probs.T, n)
        q, k = (a.reshape(n * sd, HEAD) for a in (q, k))
        hf = call_attend_gather(q, k, v, xf, wo, n)
        h, buf = call_dispatch(metas, hf, cap, ne // n)
        return h, buf

    return jax.shard_map(local, mesh=mesh, in_specs=(row, full, full, full, full, row, row), out_specs=(row, P(("dp", "sp"), None, None)), check_vma=False)
```
